32 devices in a mesh: grp: 4 (over y, x), dev: 8 (over z, core).
Axes of the slice: x: 2, y: 2, z: 4, core: 2. Of those that a mesh axis runs over, the one named last changes fastest.
Arguments:
- merged: bfloat16 [512, 4096], P('dev', 'grp'), may hold values from -90 to 90
- token_gain: float32 [4096], P('grp'), may hold values from 0.5 to 2
- expert_ids: int32 [512, 2], P('dev'), may hold values from 0 to 3, all different within a row; in each aligned block of 64 rows (0 to 63, 64 to 127, ...) at most 40 rows name the same one
- expert_gates: float32 [512, 2], P('dev'), may hold values from 0.1 to 1
- gate_proj: bfloat16 [8, 4096, 768], P('dev', 'grp'), may hold values from -0.09375 to 0.09375
- up_proj: bfloat16 [8, 4096, 768], P('dev', 'grp'), may hold values from -0.09375 to 0.09375
- down_proj: bfloat16 [8, 768, 4096], P('dev', None, 'grp'), may hold values from -0.15625 to 0.15625
Outputs:
- moe_out: bfloat16 [512, 4096], P('dev', 'grp')
The draws below stay inside these ranges and needn't reach their ends.
Inputs may be any that keep to these rules, and one draw needn't show every extreme that they name: `expert_ids`: each row names 2 different experts. Among the rows of one device no expert is named more than 40 times, and some device names one expert exactly 40 times.
All inputs are finite; a program needn't handle non-finite values.
Results may differ from the reference program's by a relative error of at most 0.019.
Values may be sent and summed in bfloat16 or wider, within the bound.
No kernel may reach another device: no remote copies, remote signals or barrier semaphores. Data moves between devices by JAX's collectives and lax.ppermute only.
A program may use at most 64 MiB of HBM per device.

```python
import math
import jax
import jax.numpy as jnp
import numpy as np
from jax import lax

D = 4096
FF = 1536
TOK_DEV = 64
TOKENS = 512
EXPERTS = 4
TOP = 2
CAP = 40
N_GRP = 4
N_DEV = 8


def draw_merged(key, part):
    first, second, third = jax.random.split(jax.random.fold_in(key, 23), 3)
    shape = (TOKENS, D)
    base = jnp.clip(jax.random.normal(first, shape, jnp.float32), -4.0, 4.0)
    row_scale = jnp.exp(jax.random.uniform(second, (TOKENS, 1), jnp.float32, 0.0, math.log(10.0)))
    ramp = jnp.exp(math.log(3.0) * jnp.arange(D, dtype=jnp.float32)[None, :] / (D - 1))
    col_scale = ramp * jnp.exp(jax.random.uniform(third, (1, D), jnp.float32, 0.0, math.log(2.0)))
    return (base * row_scale * col_scale / 3.0).astype(jnp.bfloat16)


def block_scale(own_key, extent, cuts, low, largest):
    def one(axis_at, parts):
        heights = jax.random.uniform(jax.random.fold_in(jax.random.fold_in(own_key, 6), axis_at), (parts,), jnp.float32, low / len(cuts), largest / len(cuts))
        return jnp.repeat(jnp.exp(heights), extent[axis_at] // parts).reshape((-1,) + (1,) * (len(extent) - axis_at - 1))

    factor_of = one(*cuts[0])
    for cut in cuts[1:]:
        factor_of = factor_of * one(*cut)
    return factor_of


def routed_block(stream_key, own, number, rows, amount, top, limit, skew):
    ranking = jax.random.permutation(stream_key, amount)
    heavy_load, common = load_shares(amount, rows * top, limit, skew, True), load_shares(amount, rows * top, limit, skew, False)
    places = jnp.arange(amount)

    def named(tallies, turn):
        used = int((tallies > 0).sum())
        fixed = max(1, used // 4)
        shifted = fixed + (places - fixed + turn * (used - fixed)) % max(1, amount - fixed)
        return jnp.zeros((amount,), jnp.int32).at[ranking[jnp.where(places < fixed, places, shifted)]].set(jnp.asarray(tallies, jnp.int32))

    tallies = jnp.where(number % 4 == 0, named(heavy_load, number // 4), named(common, number - number // 4 - 1))
    mixed = jax.random.permutation(jax.random.fold_in(own, 3), amount)
    source_of, sink = mixed[0:amount // 2 * 2:2], mixed[1:amount // 2 * 2:2]
    slack = jnp.minimum(tallies[source_of] - 1, limit - tallies[sink]) // 2
    slack = jnp.where((source_of == ranking[0]) | (sink == ranking[0]) | (tallies[sink] == 0), 0, jnp.maximum(slack, 0))
    shifted = jax.random.randint(jax.random.fold_in(own, 4), (amount // 2,), 0, 1 << 20) % (slack + 1)
    tallies = tallies.at[source_of].add(-shifted).at[sink].add(shifted)
    items = jnp.searchsorted(jnp.cumsum(tallies), jnp.arange(rows * top), side="right").astype(jnp.int32)
    table = items.reshape(top, rows).T
    table = table[jax.random.permutation(jax.random.fold_in(own, 1), rows)]
    turn = jax.random.randint(jax.random.fold_in(own, 2), (rows, 1), 0, top)
    return jnp.take_along_axis(table, (jnp.arange(top)[None, :] + turn) % top, axis=1)


def load_shares(amount, total, reach, lean, full):
    loads = [(1 << 20) // math.isqrt(rank ** lean) + 1 for rank in range(1, amount + 1)]
    largest = reach if full else min(reach, max(-(-total // amount), total * loads[0] // sum(loads)))
    least = 1 if total - largest >= amount - 1 else 0
    given, spare = [largest] + [least] * (amount - 1), total - largest - least * (amount - 1)
    while spare > 0:
        movable = [i for i in range(1, amount) if given[i] < largest] or [i for i in range(1, amount) if given[i] < reach]
        pool, left = sum([loads[i] for i in movable]), spare
        for i in movable:
            addition = min(reach - given[i], max(1, left * loads[i] // pool), spare)
            given[i] = given[i] + addition
            spare = spare - addition
    return np.array(given)


def scatter_about(stream_key, dims, scale, reach, pieces=(), kind=jnp.bfloat16):
    result = scale * jax.random.normal(stream_key, dims, jnp.float32)
    if pieces:
        result = result * block_scale(stream_key, dims, pieces, -0.22, 0.18)
    return jnp.clip(result, -reach, reach).astype(kind)


def setup_inputs(seed: int = 0) -> dict:
    keys = jax.random.split(jax.random.key(seed), 8)
    merged = draw_merged(jax.random.fold_in(keys[7], 71), 0)
    token_gain = jnp.clip(jnp.exp(math.log(2.0) - 1.3862944 * jax.random.uniform(keys[1], (D,), jnp.float32) ** block_scale(keys[1], (D,), ((0, 4),), -0.2, 0.2)), 0.5, 2.0)
    expert_ids_keys = jax.random.split(jax.random.fold_in(keys[2], 1), TOKENS // TOK_DEV)
    expert_ids_turns = jax.random.permutation(jax.random.fold_in(keys[2], 3), TOKENS // TOK_DEV)
    expert_ids = jax.vmap(lambda own, number: routed_block(jax.random.fold_in(keys[2], 2), own, number, TOK_DEV, EXPERTS, TOP, CAP, 1))(expert_ids_keys, expert_ids_turns).reshape((TOKENS, TOP))
    expert_gates = jnp.clip(jnp.exp(math.log(1.0) - 2.3025851 * jax.random.uniform(keys[3], (TOKENS, TOP), jnp.float32) ** block_scale(keys[3], (TOKENS, TOP), ((0, 8),), -0.2, 0.2)), 0.1, 1.0)
    gate_proj = scatter_about(keys[4], (2 * EXPERTS, D, FF // 2), D ** -0.5, 0.09375, ((0, 8), (1, 4)))
    up_proj = scatter_about(keys[5], (2 * EXPERTS, D, FF // 2), D ** -0.5, 0.09375, ((0, 8), (1, 4)))
    down_proj = scatter_about(keys[6], (2 * EXPERTS, FF // 2, D), FF ** -0.5, 0.15625, ((0, 8), (2, 4)))
    return {"merged": merged, "token_gain": token_gain, "expert_ids": expert_ids, "expert_gates": expert_gates, "gate_proj": gate_proj, "up_proj": up_proj, "down_proj": down_proj}


EPSILON = 1e-06

def half_product(token_rows, weight_mat):
    quarter = D // N_GRP
    rows = token_rows.reshape(token_rows.shape[0], N_GRP, quarter).astype(jnp.float32)
    blocks = weight_mat.reshape(N_GRP, quarter, weight_mat.shape[-1]).astype(jnp.float32)
    partial_value = jnp.einsum('rqd,qdf->rqf', rows, blocks).astype(jnp.bfloat16)
    partial_value = lax.optimization_barrier(partial_value)
    return lax.optimization_barrier(jnp.sum(partial_value.astype(jnp.float32), axis=1))

def reference(merged, token_gain, expert_ids, expert_gates, gate_proj, up_proj, down_proj):
    merged_f = merged.astype(jnp.float32)
    hidden_in = merged_f * lax.rsqrt(lax.optimization_barrier(jnp.mean(merged_f * merged_f, axis=-1, keepdims=True)) + EPSILON) * token_gain
    hidden_in = hidden_in.astype(jnp.bfloat16)
    weights = expert_gates / lax.optimization_barrier(jnp.sum(expert_gates, axis=-1, keepdims=True))
    flat_ids = expert_ids.reshape(-1)
    flat_weights = weights.reshape(-1)
    most_rows = N_DEV * CAP

    def one_expert(running, expert_index):
        hits = flat_ids == expert_index
        found_at = jnp.nonzero(hits, size=most_rows, fill_value=0)[0].astype(jnp.int32)
        route_count = jnp.sum(hits.astype(jnp.int32))
        is_live = jnp.arange(most_rows, dtype=jnp.int32) < route_count
        token_index = (found_at // TOP).astype(jnp.int32)
        token_rows = hidden_in[token_index]
        summed = jnp.zeros((most_rows, D), jnp.float32)
        for half in range(2):
            gate_val = half_product(token_rows, gate_proj[2 * expert_index + half])
            up_val = half_product(token_rows, up_proj[2 * expert_index + half])
            activity = (jax.nn.silu(gate_val) * up_val).astype(jnp.bfloat16)
            half_out = jnp.dot(activity, down_proj[2 * expert_index + half], preferred_element_type=jnp.float32).astype(jnp.bfloat16)
            summed = summed + half_out.astype(jnp.float32)
        route_scale = jnp.where(is_live, flat_weights[found_at], jnp.zeros((), jnp.float32))
        running = running.at[token_index].add(summed * route_scale[:, None])
        return (running, None)
    running, _ = lax.scan(one_expert, jnp.zeros((TOKENS, D), jnp.float32), jnp.arange(EXPERTS, dtype=jnp.int32))
    return running.astype(jnp.bfloat16)
```

```python
import functools

import jax
import jax.numpy as jnp
from jax import lax
from jax.experimental import pallas as pl
from jax.experimental.pallas import tpu as pltpu
from jax.sharding import PartitionSpec as P

EPSILON = 1e-06
LANES = 128
ROW_TILE = 8


def swap(block, axis, distance):
    count = lax.axis_size(axis)
    return lax.ppermute(block, axis, [(i, i ^ distance) for i in range(count)])


def run(kernel, outs, scratch=(), flops=0, moved=0):
    single = not isinstance(outs, (list, tuple))
    listed = [outs] if single else list(outs)
    vmem = pl.BlockSpec(memory_space=pltpu.VMEM)

    def call(*args):
        return pl.pallas_call(
            kernel,
            out_shape=listed[0] if single else listed,
            in_specs=[vmem] * len(args),
            out_specs=vmem if single else [vmem] * len(listed),
            scratch_shapes=list(scratch),
            cost_estimate=pl.CostEstimate(flops=flops, bytes_accessed=moved, transcendentals=0),
        )(*args)

    return call


def slots_of(ids, chip, experts):
    top, tokens = ids.shape
    expert = lax.broadcasted_iota(jnp.int32, (experts, tokens), 0) ^ chip
    named = jnp.zeros((experts, tokens), jnp.float32)
    for k in range(top):
        named = named + (ids[k : k + 1, :] == expert).astype(jnp.float32)
    earlier = lax.broadcasted_iota(jnp.int32, (tokens, tokens), 0) < lax.broadcasted_iota(
        jnp.int32, (tokens, tokens), 1
    )
    before = jnp.dot(
        named.astype(jnp.bfloat16), earlier.astype(jnp.bfloat16), preferred_element_type=jnp.float32
    ).astype(jnp.int32)
    return named, jnp.where(named > 0, before, -1)


def pick_kernel(experts, ids_ref, tok_ref, *refs):
    out_refs = refs[:experts]
    scratch = refs[experts]
    slots = out_refs[0].shape[0]
    tokens = tok_ref.shape[0]
    chip = lax.axis_index("dev") // 2
    _, slot = slots_of(ids_ref[...], chip, experts)
    place = lax.broadcasted_iota(jnp.int32, (slots, tokens), 0)
    for d in range(experts):
        scratch[d * slots : (d + 1) * slots, :] = (slot[d : d + 1, :] == place).astype(jnp.bfloat16)
    rows = jnp.dot(scratch[...], tok_ref[...], preferred_element_type=jnp.float32).astype(jnp.bfloat16)
    for d in range(experts):
        out_refs[d][...] = rows[d * slots : (d + 1) * slots, :]


def weigh_kernel(experts, slots, ids_ref, gates_ref, out_ref):
    top, tokens = ids_ref.shape
    chip = lax.axis_index("dev") // 2
    ids = ids_ref[...]
    gates = gates_ref[...]
    total = gates[0:1, :]
    for k in range(1, top):
        total = total + gates[k : k + 1, :]
    weights = gates / total
    named, slot = slots_of(ids, chip, experts)
    expert = lax.broadcasted_iota(jnp.int32, (experts, tokens), 0) ^ chip
    scale = jnp.zeros((experts, tokens), jnp.float32)
    for k in range(top):
        scale = scale + jnp.where(ids[k : k + 1, :] == expert, weights[k : k + 1, :], 0.0)
    place = lax.broadcasted_iota(jnp.int32, (slots, tokens), 0)
    for d in range(experts):
        block = jnp.where(slot[d : d + 1, :] == place, scale[d : d + 1, :], 0.0)
        out_ref[d * slots : (d + 1) * slots, :] = block


def hidden_kernel(experts, groups, *refs):
    own_refs = refs[:experts]
    other_ref, gain_ref, gate_ref, up_ref = refs[experts : experts + 4]
    out_refs = refs[experts + 4 : experts + 4 + groups]
    x_ref = refs[experts + 4 + groups]
    stack_ref = refs[experts + 5 + groups]
    slots = own_refs[0].shape[0]
    per = experts // groups
    part = per * 2 * slots
    width = gate_ref.shape[2]
    me = lax.axis_index("grp")
    gain = gain_ref[...]
    for d in range(experts):
        stack_ref[d] = own_refs[d][...]
    for s in range(groups):
        for j in range(per):
            d = (me ^ s) * per + j
            for c, source in enumerate((stack_ref, other_ref)):
                block = source[d].astype(jnp.float32)
                at = s * part + (j * 2 + c) * slots
                x_ref[at : at + slots, :] = (block * gain).astype(jnp.bfloat16)
                square = jnp.sum(block * block, axis=1, keepdims=True)
                high = square.astype(jnp.bfloat16).astype(jnp.float32)
                low = square - high
                lane = lax.broadcasted_iota(jnp.int32, (slots, LANES), 1)
                packed = jnp.where(lane == 0, high, jnp.where(lane == 1, low, 0.0))
                row = (j * 2 + c) * slots
                out_refs[s][row : row + slots, 2 * width : 2 * width + LANES] = packed.astype(jnp.bfloat16)
    tile = 256 if width % 256 == 0 else width
    for base, weight_ref in ((0, gate_ref), (width, up_ref)):
        for col in range(0, width, tile):
            value = jnp.dot(
                x_ref[...], weight_ref[0, :, col : col + tile], preferred_element_type=jnp.float32
            ).astype(jnp.bfloat16)
            for s in range(groups):
                out_refs[s][:, base + col : base + col + tile] = value[s * part : (s + 1) * part, :]


def activity_kernel(model_width, *refs):
    part_refs, out_ref = refs[:-1], refs[-1]
    width = out_ref.shape[1]

    def total(lo, hi):
        value = part_refs[0][:, lo:hi].astype(jnp.float32)
        for ref in part_refs[1:]:
            value = value + ref[:, lo:hi].astype(jnp.float32)
        return value

    square = jnp.sum(total(2 * width, 2 * width + LANES), axis=1, keepdims=True)
    scale = lax.rsqrt(square / model_width + EPSILON)
    gate_val = total(0, width) * scale
    up_val = total(width, 2 * width) * scale
    out_ref[...] = (gate_val / (1.0 + jnp.exp(-gate_val)) * up_val).astype(jnp.bfloat16)


def down_kernel(experts, groups, *refs):
    act_refs = refs[:groups]
    down_ref, keep_ref, send_ref, x_ref = refs[groups:]
    slots = keep_ref.shape[1]
    per = experts // groups
    part = per * 2 * slots
    me = lax.axis_index("grp")
    for s in range(groups):
        x_ref[s * part : (s + 1) * part, :] = act_refs[s][...]
    width = down_ref.shape[2]
    tile = 256 if width % 256 == 0 else width
    for col in range(0, width, tile):
        value = jnp.dot(
            x_ref[...], down_ref[0, :, col : col + tile], preferred_element_type=jnp.float32
        ).astype(jnp.bfloat16)
        for s in range(groups):
            for j in range(per):
                d = (me ^ s) * per + j
                at = s * part + j * 2 * slots
                keep_ref[d, :, col : col + tile] = value[at : at + slots, :]
                send_ref[d, :, col : col + tile] = value[at + slots : at + 2 * slots, :]


def pair_kernel(experts, keep_ref, other_ref, *out_refs):
    for d in range(experts):
        out_refs[d][...] = (
            keep_ref[d].astype(jnp.float32) + other_ref[d].astype(jnp.float32)
        ).astype(jnp.bfloat16)


def combine_kernel(experts, weigh_ref, *refs):
    back_refs, out_ref, rows_ref = refs[:experts], refs[experts], refs[experts + 1]
    slots = back_refs[0].shape[0]
    for d in range(experts):
        rows_ref[d * slots : (d + 1) * slots, :] = back_refs[d][...]
    weigh = weigh_ref[...]
    high = weigh.astype(jnp.bfloat16)
    low = (weigh - high.astype(jnp.float32)).astype(jnp.bfloat16)
    rows = rows_ref[...]
    dims = (((0,), (0,)), ((), ()))
    value = lax.dot_general(high, rows, dims, preferred_element_type=jnp.float32)
    value = value + lax.dot_general(low, rows, dims, preferred_element_type=jnp.float32)
    out_ref[...] = value.astype(jnp.bfloat16)


def body(merged, token_gain, expert_ids, expert_gates, gate_proj, up_proj, down_proj):
    tok_rows, quarter = merged.shape
    groups = lax.axis_size("grp")
    devices = lax.axis_size("dev")
    experts = devices // 2
    top = expert_ids.shape[1]
    width = gate_proj.shape[2]
    capacity = 2 * ((5 * tok_rows * top + 8 * experts - 1) // (8 * experts))
    slots = -(-capacity // ROW_TILE) * ROW_TILE
    rows = experts * 2 * slots
    part = rows // groups
    bf16, f32 = jnp.bfloat16, jnp.float32

    def like(shape, kind=bf16):
        return jax.ShapeDtypeStruct(shape, kind)

    ids = expert_ids.T
    gates = expert_gates.T
    picked = run(
        functools.partial(pick_kernel, experts),
        [like((slots, quarter))] * experts,
        [pltpu.VMEM((experts * slots, tok_rows), bf16)],
        flops=2 * experts * slots * tok_rows * quarter,
        moved=4 * experts * slots * quarter,
    )(ids, merged)
    arrived = [picked[0]] + [swap(picked[d], "dev", 2 * d) for d in range(1, experts)]
    weigh = run(
        functools.partial(weigh_kernel, experts, slots),
        like((experts * slots, tok_rows), f32),
        flops=2 * experts * slots * tok_rows * 128,
        moved=4 * experts * slots * tok_rows,
    )(ids, gates)
    other = swap(jnp.stack(arrived), "dev", 1)
    parts = run(
        functools.partial(hidden_kernel, experts, groups),
        [like((part, 2 * width + LANES))] * groups,
        [pltpu.VMEM((rows, quarter), bf16), pltpu.VMEM((experts, slots, quarter), bf16)],
        flops=4 * rows * quarter * width,
        moved=4 * quarter * width,
    )(*arrived, other, token_gain.reshape(1, -1), gate_proj, up_proj)
    parts = [parts[0]] + [swap(parts[s], "grp", s) for s in range(1, groups)]
    active = run(
        functools.partial(activity_kernel, quarter * groups),
        like((part, width)),
        flops=20 * part * width,
        moved=2 * part * width * 9,
    )(*parts)
    actives = [active] + [swap(active, "grp", s) for s in range(1, groups)]
    keep, send = run(
        functools.partial(down_kernel, experts, groups),
        [like((experts, slots, quarter))] * 2,
        [pltpu.VMEM((rows, width), bf16)],
        flops=2 * rows * quarter * width,
        moved=2 * quarter * width,
    )(*actives, down_proj)
    send = swap(send, "dev", 1)
    paired = run(
        functools.partial(pair_kernel, experts),
        [like((slots, quarter))] * experts,
        flops=experts * slots * quarter,
        moved=6 * experts * slots * quarter,
    )(keep, send)
    back = [paired[0]] + [swap(paired[d], "dev", 2 * d) for d in range(1, experts)]
    return run(
        functools.partial(combine_kernel, experts),
        like((tok_rows, quarter)),
        [pltpu.VMEM((experts * slots, quarter), bf16)],
        flops=4 * tok_rows * experts * slots * quarter,
        moved=2 * experts * slots * quarter,
    )(weigh, *back)


def solution(mesh):
    return jax.shard_map(
        body,
        mesh=mesh,
        in_specs=(
            P("dev", "grp"),
            P("grp"),
            P("dev", None),
            P("dev", None),
            P("dev", "grp", None),
            P("dev", "grp", None),
            P("dev", None, "grp"),
        ),
        out_specs=P("dev", "grp"),
        check_vma=False,
    )
```

```python
import functools
import math

import jax
import jax.numpy as jnp
from jax import lax
from jax.experimental import pallas as pl
from jax.experimental.pallas import tpu as pltpu
from jax.sharding import PartitionSpec as P

EPSILON = 1e-06
LANES = 128
ROW_TILE = 8
GRANT = 60 << 20


def swap(block, axis, distance):
    count = lax.axis_size(axis)
    return lax.ppermute(block, axis, [(i, i ^ distance) for i in range(count)])


def run(kernel, outs, scratch=(), flops=0, moved=0):
    single = not isinstance(outs, (list, tuple))
    listed = [outs] if single else list(outs)
    vmem = pl.BlockSpec(memory_space=pltpu.VMEM)

    def call(*args):
        held = sum(a.size * a.dtype.itemsize for a in (*args, *listed))
        held += sum(math.prod(a.shape) * jnp.dtype(a.dtype).itemsize for a in scratch)
        return pl.pallas_call(
            kernel,
            out_shape=listed[0] if single else listed,
            in_specs=[vmem] * len(args),
            out_specs=vmem if single else [vmem] * len(listed),
            scratch_shapes=list(scratch),
            compiler_params=pltpu.CompilerParams(vmem_limit_bytes=min(2 * held + (8 << 20), GRANT)),
            cost_estimate=pl.CostEstimate(flops=flops, bytes_accessed=moved, transcendentals=0),
        )(*args)

    return call


def slots_of(ids, chip, experts):
    top, tokens = ids.shape
    expert = lax.broadcasted_iota(jnp.int32, (experts, tokens), 0) ^ chip
    named = jnp.zeros((experts, tokens), jnp.float32)
    for k in range(top):
        named = named + (ids[k : k + 1, :] == expert).astype(jnp.float32)
    earlier = lax.broadcasted_iota(jnp.int32, (tokens, tokens), 0) < lax.broadcasted_iota(
        jnp.int32, (tokens, tokens), 1
    )
    before = jnp.dot(
        named.astype(jnp.bfloat16), earlier.astype(jnp.bfloat16), preferred_element_type=jnp.float32
    ).astype(jnp.int32)
    return named, jnp.where(named > 0, before, -1)


def pick_kernel(experts, ids_ref, tok_ref, *refs):
    out_refs = refs[:experts]
    scratch = refs[experts]
    slots = out_refs[0].shape[0]
    tokens = tok_ref.shape[0]
    chip = lax.axis_index("dev") // 2
    _, slot = slots_of(ids_ref[...], chip, experts)
    place = lax.broadcasted_iota(jnp.int32, (slots, tokens), 0)
    for d in range(experts):
        scratch[d * slots : (d + 1) * slots, :] = (slot[d : d + 1, :] == place).astype(jnp.bfloat16)
    rows = jnp.dot(scratch[...], tok_ref[...], preferred_element_type=jnp.float32).astype(jnp.bfloat16)
    for d in range(experts):
        out_refs[d][...] = rows[d * slots : (d + 1) * slots, :]


def weigh_kernel(experts, slots, ids_ref, gates_ref, out_ref):
    top, tokens = ids_ref.shape
    chip = lax.axis_index("dev") // 2
    ids = ids_ref[...]
    gates = gates_ref[...]
    total = gates[0:1, :]
    for k in range(1, top):
        total = total + gates[k : k + 1, :]
    weights = gates / total
    named, slot = slots_of(ids, chip, experts)
    expert = lax.broadcasted_iota(jnp.int32, (experts, tokens), 0) ^ chip
    scale = jnp.zeros((experts, tokens), jnp.float32)
    for k in range(top):
        scale = scale + jnp.where(ids[k : k + 1, :] == expert, weights[k : k + 1, :], 0.0)
    place = lax.broadcasted_iota(jnp.int32, (slots, tokens), 0)
    for d in range(experts):
        block = jnp.where(slot[d : d + 1, :] == place, scale[d : d + 1, :], 0.0)
        out_ref[d * slots : (d + 1) * slots, :] = block


def hidden_kernel(experts, groups, *refs):
    own_refs = refs[:experts]
    other_ref, gain_ref, gate_ref, up_ref = refs[experts : experts + 4]
    out_refs = refs[experts + 4 : experts + 4 + groups]
    x_ref = refs[experts + 4 + groups]
    stack_ref = refs[experts + 5 + groups]
    slots = own_refs[0].shape[0]
    per = experts // groups
    part = per * 2 * slots
    width = gate_ref.shape[2]
    me = lax.axis_index("grp")
    gain = gain_ref[...]
    for d in range(experts):
        stack_ref[d] = own_refs[d][...]
    for s in range(groups):
        for j in range(per):
            d = (me ^ s) * per + j
            for c, source in enumerate((stack_ref, other_ref)):
                block = source[d].astype(jnp.float32)
                at = s * part + (j * 2 + c) * slots
                x_ref[at : at + slots, :] = (block * gain).astype(jnp.bfloat16)
                square = jnp.sum(block * block, axis=1, keepdims=True)
                high = square.astype(jnp.bfloat16).astype(jnp.float32)
                low = square - high
                lane = lax.broadcasted_iota(jnp.int32, (slots, LANES), 1)
                packed = jnp.where(lane == 0, high, jnp.where(lane == 1, low, 0.0))
                row = (j * 2 + c) * slots
                out_refs[s][row : row + slots, 2 * width : 2 * width + LANES] = packed.astype(jnp.bfloat16)
    tile = 256 if width % 256 == 0 else width
    for base, weight_ref in ((0, gate_ref), (width, up_ref)):
        for col in range(0, width, tile):
            value = jnp.dot(
                x_ref[...], weight_ref[0, :, col : col + tile], preferred_element_type=jnp.float32
            ).astype(jnp.bfloat16)
            for s in range(groups):
                out_refs[s][:, base + col : base + col + tile] = value[s * part : (s + 1) * part, :]


def activity_kernel(model_width, *refs):
    part_refs, out_ref = refs[:-1], refs[-1]
    width = out_ref.shape[1]

    def total(lo, hi):
        value = part_refs[0][:, lo:hi].astype(jnp.float32)
        for ref in part_refs[1:]:
            value = value + ref[:, lo:hi].astype(jnp.float32)
        return value

    square = jnp.sum(total(2 * width, 2 * width + LANES), axis=1, keepdims=True)
    scale = lax.rsqrt(square / model_width + EPSILON)
    gate_val = total(0, width) * scale
    up_val = total(width, 2 * width) * scale
    out_ref[...] = (gate_val / (1.0 + jnp.exp(-gate_val)) * up_val).astype(jnp.bfloat16)


def down_kernel(experts, groups, *refs):
    act_refs = refs[:groups]
    down_ref, keep_ref, send_ref, x_ref = refs[groups:]
    slots = keep_ref.shape[1]
    per = experts // groups
    part = per * 2 * slots
    me = lax.axis_index("grp")
    for s in range(groups):
        x_ref[s * part : (s + 1) * part, :] = act_refs[s][...]
    width = down_ref.shape[2]
    tile = 256 if width % 256 == 0 else width
    for col in range(0, width, tile):
        value = jnp.dot(
            x_ref[...], down_ref[0, :, col : col + tile], preferred_element_type=jnp.float32
        ).astype(jnp.bfloat16)
        for s in range(groups):
            for j in range(per):
                d = (me ^ s) * per + j
                at = s * part + j * 2 * slots
                keep_ref[d, :, col : col + tile] = value[at : at + slots, :]
                send_ref[d, :, col : col + tile] = value[at + slots : at + 2 * slots, :]


def pair_kernel(experts, keep_ref, other_ref, *out_refs):
    for d in range(experts):
        out_refs[d][...] = (
            keep_ref[d].astype(jnp.float32) + other_ref[d].astype(jnp.float32)
        ).astype(jnp.bfloat16)


def combine_kernel(experts, weigh_ref, *refs):
    back_refs, out_ref, rows_ref = refs[:experts], refs[experts], refs[experts + 1]
    slots = back_refs[0].shape[0]
    for d in range(experts):
        rows_ref[d * slots : (d + 1) * slots, :] = back_refs[d][...]
    weigh = weigh_ref[...]
    high = weigh.astype(jnp.bfloat16)
    low = (weigh - high.astype(jnp.float32)).astype(jnp.bfloat16)
    rows = rows_ref[...]
    dims = (((0,), (0,)), ((), ()))
    value = lax.dot_general(high, rows, dims, preferred_element_type=jnp.float32)
    value = value + lax.dot_general(low, rows, dims, preferred_element_type=jnp.float32)
    out_ref[...] = value.astype(jnp.bfloat16)


def body(merged, token_gain, expert_ids, expert_gates, gate_proj, up_proj, down_proj):
    tok_rows, quarter = merged.shape
    groups = lax.axis_size("grp")
    devices = lax.axis_size("dev")
    experts = devices // 2
    top = expert_ids.shape[1]
    width = gate_proj.shape[2]
    capacity = 2 * ((5 * tok_rows * top + 8 * experts - 1) // (8 * experts))
    slots = -(-capacity // ROW_TILE) * ROW_TILE
    rows = experts * 2 * slots
    part = rows // groups
    bf16, f32 = jnp.bfloat16, jnp.float32

    def like(shape, kind=bf16):
        return jax.ShapeDtypeStruct(shape, kind)

    ids = expert_ids.T
    gates = expert_gates.T
    picked = run(
        functools.partial(pick_kernel, experts),
        [like((slots, quarter))] * experts,
        [pltpu.VMEM((experts * slots, tok_rows), bf16)],
        flops=2 * experts * slots * tok_rows * quarter,
        moved=4 * experts * slots * quarter,
    )(ids, merged)
    arrived = [picked[0]] + [swap(picked[d], "dev", 2 * d) for d in range(1, experts)]
    weigh = run(
        functools.partial(weigh_kernel, experts, slots),
        like((experts * slots, tok_rows), f32),
        flops=2 * experts * slots * tok_rows * 128,
        moved=4 * experts * slots * tok_rows,
    )(ids, gates)
    other = swap(jnp.stack(arrived), "dev", 1)
    parts = run(
        functools.partial(hidden_kernel, experts, groups),
        [like((part, 2 * width + LANES))] * groups,
        [pltpu.VMEM((rows, quarter), bf16), pltpu.VMEM((experts, slots, quarter), bf16)],
        flops=4 * rows * quarter * width,
        moved=4 * quarter * width,
    )(*arrived, other, token_gain.reshape(1, -1), gate_proj, up_proj)
    parts = [parts[0]] + [swap(parts[s], "grp", s) for s in range(1, groups)]
    active = run(
        functools.partial(activity_kernel, quarter * groups),
        like((part, width)),
        flops=20 * part * width,
        moved=2 * part * width * 9,
    )(*parts)
    actives = [active] + [swap(active, "grp", s) for s in range(1, groups)]
    keep, send = run(
        functools.partial(down_kernel, experts, groups),
        [like((experts, slots, quarter))] * 2,
        [pltpu.VMEM((rows, width), bf16)],
        flops=2 * rows * quarter * width,
        moved=2 * quarter * width,
    )(*actives, down_proj)
    send = swap(send, "dev", 1)
    paired = run(
        functools.partial(pair_kernel, experts),
        [like((slots, quarter))] * experts,
        flops=experts * slots * quarter,
        moved=6 * experts * slots * quarter,
    )(keep, send)
    back = [paired[0]] + [swap(paired[d], "dev", 2 * d) for d in range(1, experts)]
    return run(
        functools.partial(combine_kernel, experts),
        like((tok_rows, quarter)),
        [pltpu.VMEM((experts * slots, quarter), bf16)],
        flops=4 * tok_rows * experts * slots * quarter,
        moved=2 * experts * slots * quarter,
    )(weigh, *back)


def solution(mesh):
    return jax.shard_map(
        body,
        mesh=mesh,
        in_specs=(
            P("dev", "grp"),
            P("grp"),
            P("dev", None),
            P("dev", None),
            P("dev", "grp", None),
            P("dev", "grp", None),
            P("dev", None, "grp"),
        ),
        out_specs=P("dev", "grp"),
        check_vma=False,
    )
```
